32 devices in a mesh: py: 8 (over z, x), px: 4 (over y, core).
Axes of the slice: x: 2, y: 2, z: 4, core: 2. Of those that a mesh axis runs over, the one named last changes fastest.
Arguments:
- density: float32 [256, 128, 128], P('py', 'px'), may hold values from 0.5 to 2
- conductance: float32 [256, 128, 128], P('py', 'px'), may hold values from 0.03 to 0.22
- source: float32 [256, 128, 128], P('py', 'px'), may hold values from -0.2 to 0.2
Outputs:
- anomaly: float32 [256, 128, 128], P('py', 'px')
- density_end: float32 [256, 128, 128], P('py', 'px')
The draws below stay inside these ranges and needn't reach their ends.
All inputs are finite; a program needn't handle non-finite values.
Results may differ from the reference program's by a relative error of at most 0.00002.
Values sent between devices are 32-bit elements; how exact they have to be, the bound alone decides.
No kernel may reach another device: no remote copies, remote signals or barrier semaphores. Data moves between devices by JAX's collectives and lax.ppermute only.
A program may use at most 64 MiB of HBM per device.

```python
import jax
import jax.numpy as jnp
from jax import lax

GRID_Y = 256
GRID_X = 128
LEVELS = 128
STEPS = 6


def steps_of(rng, shape, cuts, least, high):
    loudness, own = 1.0, jax.random.fold_in(rng, 6)
    for dim, shards_of in cuts:
        steps = jnp.exp(jax.random.uniform(jax.random.fold_in(own, dim), (shards_of,), jnp.float32, least / len(cuts), high / len(cuts)))
        loudness = loudness * jnp.repeat(steps, shape[dim] // shards_of).reshape([-1 if axis == dim else 1 for axis in range(len(shape))])
    return loudness


def setup_inputs(seed: int = 0) -> dict:
    key_list = jax.random.split(jax.random.key(seed), 4)
    return {
        "density": jnp.clip(0.5 + 1.5 * jax.random.uniform(key_list[0], (GRID_Y, GRID_X, LEVELS), jnp.float32) ** steps_of(key_list[0], (GRID_Y, GRID_X, LEVELS), ((0, 8), (1, 4)), -0.2, 0.2), 0.5, 2.0),
        "conductance": jnp.clip(0.03 + 0.19 * jax.random.uniform(key_list[1], (GRID_Y, GRID_X, LEVELS), jnp.float32) ** steps_of(key_list[1], (GRID_Y, GRID_X, LEVELS), ((0, 8), (1, 4)), -0.2, 0.2), 0.03, 0.22),
        "source": jnp.clip(jax.random.uniform(key_list[2], (GRID_Y, GRID_X, LEVELS), jnp.float32, -0.2, 0.2) * steps_of(key_list[2], (GRID_Y, GRID_X, LEVELS), ((0, 8), (1, 4)), -0.4, 0.0), -0.2, 0.2),
    }


def strip_edges(values, dims):
    for dim in dims:
        values = lax.slice_in_dim(values, 1, values.shape[dim] - 1, axis=dim)
    return values

def neighbour(values, dim, start, dims):
    others = [other for other in dims if other != dim]
    values = strip_edges(values, others)
    return lax.slice_in_dim(values, start, start + values.shape[dim] - 2, axis=dim)

def one_step(padded, conductance, source):
    middle = strip_edges(padded, (0, 1))
    lower = [neighbour(padded, dim, 0, (0, 1)) for dim in (0, 1)]
    upper = [neighbour(padded, dim, 2, (0, 1)) for dim in (0, 1)]
    spread = lower[0] + upper[0] + lower[1] + upper[1] - 4.0 * middle
    return middle + conductance * spread + source

def reference(density, conductance, source):
    for step in range(STEPS):
        density = one_step(jnp.pad(density, ((1, 1), (1, 1), (0, 0)), mode='constant'), conductance, source)
    line_mean = lax.optimization_barrier(jnp.mean(density, axis=0, keepdims=True))
    centred = density - line_mean
    line_variance = lax.optimization_barrier(jnp.mean(centred * centred, axis=0, keepdims=True))
    anomaly = centred * lax.rsqrt(line_variance + 0.0001)
    return (anomaly, density)
```

```python
import jax
import jax.numpy as jnp
from jax import lax
from jax.sharding import PartitionSpec as P

STEPS = 6


def exchange(to_upper, to_lower, axis):
    count = lax.axis_size(axis)
    up = [(i, i + 1) for i in range(count - 1)]
    down = [(i + 1, i) for i in range(count - 1)]
    return lax.ppermute(to_upper, axis, up), lax.ppermute(to_lower, axis, down)


def cut(values, start, stop, dim):
    return lax.slice_in_dim(values, start, stop, axis=dim)


def with_halo(density, conductance, source, axis, dim):
    deep, less = STEPS, STEPS - 1
    size = density.shape[dim]
    parts = (density, conductance, source)
    depths = (deep, less, less)
    tail = jnp.concatenate([cut(v, size - w, size, dim) for v, w in zip(parts, depths)], dim)
    head = jnp.concatenate([cut(v, 0, w, dim) for v, w in zip(parts, depths)], dim)
    lower, upper = exchange(tail, head, axis)
    wide, at = [], 0
    for v, w in zip(parts, depths):
        edge = deep - w
        pads = [(0, 0)] * v.ndim
        pads[dim] = (edge, edge)
        joined = jnp.concatenate([cut(lower, at, at + w, dim), v, cut(upper, at, at + w, dim)], dim)
        wide.append(jnp.pad(joined, pads))
        at += w
    return wide


def strip(values):
    return values[1:-1, 1:-1]


def one_step(padded, conductance, source):
    middle = strip(padded)
    spread = (
        padded[:-2, 1:-1] + padded[2:, 1:-1] + padded[1:-1, :-2] + padded[1:-1, 2:] - 4.0 * middle
    )
    return middle + conductance * spread + source


def line_stats(density):
    rows = density.shape[0]
    mean = jnp.mean(density, axis=0)
    off = density - mean[None]
    stats = jnp.stack([mean, jnp.sum(off * off, axis=0)])
    count = lax.axis_size("py")
    hop = 1
    while hop < count:
        other = lax.ppermute(stats, "py", [(i, i ^ hop) for i in range(count)])
        gap = other[0] - stats[0]
        stats = jnp.stack(
            [
                0.5 * (stats[0] + other[0]),
                stats[1] + other[1] + gap * gap * (0.5 * rows * hop),
            ]
        )
        hop *= 2
    return stats[0], stats[1] / (rows * count)


def per_device(density, conductance, source):
    parts = with_halo(density, conductance, source, "py", 0)
    padded, conductance, source = with_halo(*parts, "px", 1)
    for _ in range(STEPS):
        conductance, source = strip(conductance), strip(source)
        padded = one_step(padded, conductance, source)
    mean, variance = line_stats(padded)
    anomaly = (padded - mean[None]) * lax.rsqrt(variance + 0.0001)[None]
    return (anomaly, padded)


def solution(mesh):
    spec = P("py", "px", None)
    return jax.shard_map(
        per_device, mesh=mesh, in_specs=(spec,) * 3, out_specs=(spec,) * 2, check_vma=False
    )
```

```python
import jax
import jax.numpy as jnp
from jax import lax
from jax.experimental import pallas as pl
from jax.experimental.pallas import tpu as pltpu
from jax.sharding import PartitionSpec as P

STEPS = 6
LESS = STEPS - 1
TILE = 8
DEPTHS = (STEPS, LESS, LESS)
STARTS = (0, STEPS, STEPS + LESS)
PACKED = STEPS + 2 * LESS


def corner_runs():
    runs, at = [], 0
    for field, depth in enumerate(DEPTHS):
        for away in range(1, depth):
            runs.append((field, away, depth - away, at))
            at += depth - away
    return runs, -(-at // TILE) * TILE


def pack_kernel(d, c, s, y_hi, y_lo, x_hi, x_lo, hh, hl, lh, ll):
    fields = (d, c, s)
    rows, cols, _ = d.shape
    for ref, depth, at in zip(fields, DEPTHS, STARTS):
        y_hi[at : at + depth] = ref[rows - depth : rows]
        y_lo[at : at + depth] = ref[0:depth]
        x_hi[:, at : at + depth, :] = ref[:, cols - depth : cols, :]
        x_lo[:, at : at + depth, :] = ref[:, 0:depth, :]
    runs, _ = corner_runs()
    for field, away, size, at in runs:
        ref = fields[field]
        hh[at : at + size, :] = ref[rows - away, cols - size : cols, :]
        hl[at : at + size, :] = ref[rows - away, 0:size, :]
        lh[at : at + size, :] = ref[away - 1, cols - size : cols, :]
        ll[at : at + size, :] = ref[away - 1, 0:size, :]


def step_kernel(
    d, c, s, from_lo, from_hi, from_left, from_right, ll, lr, hl, hr, end, stats, p, q, cw, sw
):
    rows, cols, _ = d.shape
    left, right = TILE, TILE + cols
    top, low = STEPS, STEPS + rows
    for ref, wide, depth, at in zip((d, c, s), (p, cw, sw), DEPTHS, STARTS):
        wide[top:low, left:right, :] = ref[...]
        wide[top - depth : top, left:right, :] = from_lo[at : at + depth]
        wide[low : low + depth, left:right, :] = from_hi[at : at + depth]
        wide[top:low, left - depth : left, :] = from_left[:, at : at + depth, :]
        wide[top:low, right : right + depth, :] = from_right[:, at : at + depth, :]
    runs, _ = corner_runs()
    for field, away, size, at in runs:
        wide = (p, cw, sw)[field]
        wide[top - away, left - size : left, :] = ll[at : at + size, :]
        wide[top - away, right : right + size, :] = lr[at : at + size, :]
        wide[low + away - 1, left - size : left, :] = hl[at : at + size, :]
        wide[low + away - 1, right : right + size, :] = hr[at : at + size, :]

    width = cols + 2 * TILE
    old, new = p, q
    for step in range(STEPS - 1):
        first, count = step + 1, rows + 2 * (STEPS - 1 - step)

        def pair(i, _, old=old, new=new, first=first):
            for k in range(2):
                r = first + 2 * i + k
                mid = old[r]
                around = pltpu.roll(mid, 1, 0) + pltpu.roll(mid, width - 1, 0)
                spread = old[r - 1] + old[r + 1] + around - 4.0 * mid
                new[r] = mid + cw[r] * spread + sw[r]
            return 0

        lax.fori_loop(0, count // 2, pair, 0)
        old, new = new, old

    def last(i, total):
        for k in range(2):
            r = top + 2 * i + k
            mid = old[r]
            around = pltpu.roll(mid, 1, 0) + pltpu.roll(mid, width - 1, 0)
            spread = old[r - 1] + old[r + 1] + around - 4.0 * mid
            later = (mid + cw[r] * spread + sw[r])[left:right]
            end[2 * i + k] = later
            total = total + later
        return total

    zero = jnp.zeros(d.shape[1:], jnp.float32)
    mean = lax.fori_loop(0, rows // 2, last, zero) * (1.0 / rows)

    def squares(i, total):
        for k in range(2):
            off = end[2 * i + k] - mean
            total = total + off * off
        return total

    stats[0] = mean
    stats[1] = lax.fori_loop(0, rows // 2, squares, zero)


def neighbours(packs):
    ny, nx = lax.axis_size("py"), lax.axis_size("px")
    moves = ((1, 0), (-1, 0), (0, 1), (0, -1), (1, 1), (1, -1), (-1, 1), (-1, -1))
    got = []
    for pack, (dy, dx) in zip(packs, moves):
        pairs = [
            (y * nx + x, (y + dy) * nx + x + dx)
            for y in range(ny)
            for x in range(nx)
            if 0 <= y + dy < ny and 0 <= x + dx < nx
        ]
        got.append(lax.ppermute(pack, ("py", "px"), pairs))
    return got


def combine(stats, rows):
    count = lax.axis_size("py")
    hop = 1
    while hop < count:
        other = lax.ppermute(stats, "py", [(i, i ^ hop) for i in range(count)])
        gap = other[0] - stats[0]
        stats = jnp.stack(
            [
                0.5 * (stats[0] + other[0]),
                stats[1] + other[1] + gap * gap * (0.5 * rows * hop),
            ]
        )
        hop *= 2
    return stats[0], stats[1] / (rows * count)


def per_device(density, conductance, source):
    rows, cols, levels = density.shape
    f32 = jnp.float32
    _, corner = corner_runs()
    shape = pltpu.VMEM
    near = lambda v: pltpu.with_memory_space_constraint(v, pltpu.VMEM)
    packs = pl.pallas_call(
        pack_kernel,
        out_shape=[shape((PACKED, cols, levels), f32)] * 2
        + [shape((rows, PACKED, levels), f32)] * 2
        + [shape((corner, levels), f32)] * 4,
        name="pack",
    )(density, conductance, source)
    got = [near(v) for v in neighbours(packs)]
    wide = (rows + 2 * STEPS, cols + 2 * TILE, levels)
    end, stats = pl.pallas_call(
        step_kernel,
        out_shape=[shape(density.shape, f32), shape((2, cols, levels), f32)],
        in_specs=[pl.BlockSpec(memory_space=pltpu.VMEM)] * 11,
        scratch_shapes=[pltpu.VMEM(wide, f32)] * 4,
        name="steps",
    )(density, conductance, source, *got)
    mean, variance = combine(stats, rows)
    anomaly = (end - mean[None]) * lax.rsqrt(variance + 0.0001)[None]
    return (anomaly, end)


def solution(mesh):
    spec = P("py", "px", None)
    return jax.shard_map(
        per_device, mesh=mesh, in_specs=(spec,) * 3, out_specs=(spec,) * 2, check_vma=False
    )
```

```python
import jax
import jax.numpy as jnp
from jax import lax
from jax.experimental import pallas as pl
from jax.experimental.pallas import tpu as pltpu
from jax.sharding import PartitionSpec as P

STEPS = 6
LESS = STEPS - 1
TILE = 8
DEPTHS = (STEPS, LESS, LESS)
STARTS = (0, STEPS, STEPS + LESS)
PACKED = STEPS + 2 * LESS


def corner_runs():
    runs, at = [], 0
    for field, depth in enumerate(DEPTHS):
        for away in range(1, depth):
            runs.append((field, away, depth - away, at))
            at += depth - away
    return runs, -(-at // TILE) * TILE


def pack_kernel(d, c, s, y_hi, y_lo, x_hi, x_lo):
    rows, cols, _ = d.shape
    for ref, depth, at in zip((d, c, s), DEPTHS, STARTS):
        y_hi[at : at + depth] = ref[rows - depth : rows]
        y_lo[at : at + depth] = ref[0:depth]
        x_hi[:, at : at + depth, :] = ref[:, cols - depth : cols, :]
        x_lo[:, at : at + depth, :] = ref[:, 0:depth, :]


def corner_kernel(from_lo, from_hi, to_right, to_left):
    cols = from_lo.shape[1]
    runs, corner = corner_runs()
    for field, away, size, at in runs:
        low = STARTS[field] + DEPTHS[field] - away
        high = STARTS[field] + away - 1
        for halo, row, to in ((from_lo, low, at), (from_hi, high, corner + at)):
            to_right[to : to + size, :] = halo[row, cols - size : cols, :]
            to_left[to : to + size, :] = halo[row, 0:size, :]


def step_kernel(
    d, c, s, from_lo, from_hi, from_left, from_right, cl, cr, end, stats, p, q, cw, sw
):
    rows, cols, _ = d.shape
    left, right = TILE, TILE + cols
    top, low = STEPS, STEPS + rows
    for ref, wide, depth, at in zip((d, c, s), (p, cw, sw), DEPTHS, STARTS):
        wide[top:low, left:right, :] = ref[...]
        wide[top - depth : top, left:right, :] = from_lo[at : at + depth]
        wide[low : low + depth, left:right, :] = from_hi[at : at + depth]
        wide[top:low, left - depth : left, :] = from_left[:, at : at + depth, :]
        wide[top:low, right : right + depth, :] = from_right[:, at : at + depth, :]
    runs, corner = corner_runs()
    for field, away, size, at in runs:
        also = corner + at
        wide = (p, cw, sw)[field]
        wide[top - away, left - size : left, :] = cl[at : at + size, :]
        wide[top - away, right : right + size, :] = cr[at : at + size, :]
        wide[low + away - 1, left - size : left, :] = cl[also : also + size, :]
        wide[low + away - 1, right : right + size, :] = cr[also : also + size, :]

    width = cols + 2 * TILE
    old, new = p, q
    for step in range(STEPS - 1):
        first, count = step + 1, rows + 2 * (STEPS - 1 - step)

        def pair(i, _, old=old, new=new, first=first):
            for k in range(2):
                r = first + 2 * i + k
                mid = old[r]
                around = pltpu.roll(mid, 1, 0) + pltpu.roll(mid, width - 1, 0)
                spread = old[r - 1] + old[r + 1] + around - 4.0 * mid
                new[r] = mid + cw[r] * spread + sw[r]
            return 0

        lax.fori_loop(0, count // 2, pair, 0)
        old, new = new, old

    def last(i, total):
        for k in range(2):
            r = top + 2 * i + k
            mid = old[r]
            around = pltpu.roll(mid, 1, 0) + pltpu.roll(mid, width - 1, 0)
            spread = old[r - 1] + old[r + 1] + around - 4.0 * mid
            later = (mid + cw[r] * spread + sw[r])[left:right]
            end[2 * i + k] = later
            total = total + later
        return total

    zero = jnp.zeros(d.shape[1:], jnp.float32)
    mean = lax.fori_loop(0, rows // 2, last, zero) * (1.0 / rows)

    def squares(i, total):
        for k in range(2):
            off = end[2 * i + k] - mean
            total = total + off * off
        return total

    stats[0] = mean
    stats[1] = lax.fori_loop(0, rows // 2, squares, zero)


def exchange(to_upper, to_lower, axis):
    count = lax.axis_size(axis)
    up = [(i, i + 1) for i in range(count - 1)]
    down = [(i + 1, i) for i in range(count - 1)]
    got = lax.ppermute(to_upper, axis, up), lax.ppermute(to_lower, axis, down)
    return [pltpu.with_memory_space_constraint(v, pltpu.VMEM) for v in got]


def combine(stats, rows):
    count = lax.axis_size("py")
    hop = 1
    while hop < count:
        other = lax.ppermute(stats, "py", [(i, i ^ hop) for i in range(count)])
        gap = other[0] - stats[0]
        stats = jnp.stack(
            [
                0.5 * (stats[0] + other[0]),
                stats[1] + other[1] + gap * gap * (0.5 * rows * hop),
            ]
        )
        hop *= 2
    return stats[0], stats[1] / (rows * count)


def per_device(density, conductance, source):
    rows, cols, levels = density.shape
    f32 = jnp.float32
    _, corner = corner_runs()
    shape = pltpu.VMEM
    y_hi, y_lo, x_hi, x_lo = pl.pallas_call(
        pack_kernel,
        out_shape=[shape((PACKED, cols, levels), f32)] * 2
        + [shape((rows, PACKED, levels), f32)] * 2,
        name="pack",
    )(density, conductance, source)
    y_got = exchange(y_hi, y_lo, "py")
    x_got = exchange(x_hi, x_lo, "px")
    corners = pl.pallas_call(
        corner_kernel,
        out_shape=[shape((2 * corner, levels), f32)] * 2,
        in_specs=[pl.BlockSpec(memory_space=pltpu.VMEM)] * 2,
        name="corners",
    )(*y_got)
    got = y_got + x_got + exchange(*corners, "px")
    wide = (rows + 2 * STEPS, cols + 2 * TILE, levels)
    end, stats = pl.pallas_call(
        step_kernel,
        out_shape=[shape(density.shape, f32), shape((2, cols, levels), f32)],
        scratch_shapes=[pltpu.VMEM(wide, f32)] * 4,
        name="steps",
    )(density, conductance, source, *got)
    mean, variance = combine(stats, rows)
    anomaly = (end - mean[None]) * lax.rsqrt(variance + 0.0001)[None]
    return (anomaly, end)


def solution(mesh):
    spec = P("py", "px", None)
    return jax.shard_map(
        per_device, mesh=mesh, in_specs=(spec,) * 3, out_specs=(spec,) * 2, check_vma=False
    )
```

```python
import jax
import jax.numpy as jnp
from jax import lax
from jax.experimental import pallas as pl
from jax.experimental.pallas import tpu as pltpu
from jax.sharding import PartitionSpec as P

STEPS = 6
LESS = STEPS - 1
TILE = 8
DEPTHS = (STEPS, LESS, LESS)
STARTS = (0, STEPS, STEPS + LESS)
PACKED = STEPS + 2 * LESS


def corner_runs():
    runs, at = [], 0
    for field, depth in enumerate(DEPTHS):
        for away in range(1, depth):
            runs.append((field, away, depth - away, at))
            at += depth - away
    return runs, -(-at // TILE) * TILE


def y_pack_kernel(d, c, s, y_hi, y_lo, sems):
    rows = d.shape[0]
    copies = []
    for ref, depth, at in zip((d, c, s), DEPTHS, STARTS):
        for out, first in ((y_hi, rows - depth), (y_lo, 0)):
            copies.append(
                pltpu.make_async_copy(
                    ref.at[pl.ds(first, depth)], out.at[pl.ds(at, depth)], sems.at[len(copies)]
                )
            )
    for copy in copies:
        copy.start()
    for copy in copies:
        copy.wait()


def x_pack_kernel(d, c, s, x_hi, x_lo):
    cols = d.shape[1]
    for ref, depth, at in zip((d, c, s), DEPTHS, STARTS):
        x_hi[:, at : at + depth, :] = ref[:, cols - depth : cols, :]
        x_lo[:, at : at + depth, :] = ref[:, 0:depth, :]


def corner_kernel(from_lo, from_hi, to_right, to_left):
    cols = from_lo.shape[1]
    runs, corner = corner_runs()
    for field, away, size, at in runs:
        low = STARTS[field] + DEPTHS[field] - away
        high = STARTS[field] + away - 1
        for halo, row, to in ((from_lo, low, at), (from_hi, high, corner + at)):
            to_right[to : to + size, :] = halo[row, cols - size : cols, :]
            to_left[to : to + size, :] = halo[row, 0:size, :]


def step_kernel(
    d, c, s, from_lo, from_hi, from_left, from_right, cl, cr, end, stats, p, q, cw, sw
):
    rows, cols, _ = d.shape
    left, right = TILE, TILE + cols
    top, low = STEPS, STEPS + rows
    for ref, wide, depth, at in zip((d, c, s), (p, cw, sw), DEPTHS, STARTS):
        wide[top:low, left:right, :] = ref[...]
        wide[top - depth : top, left:right, :] = from_lo[at : at + depth]
        wide[low : low + depth, left:right, :] = from_hi[at : at + depth]
        wide[top:low, left - depth : left, :] = from_left[:, at : at + depth, :]
        wide[top:low, right : right + depth, :] = from_right[:, at : at + depth, :]
    runs, corner = corner_runs()
    for field, away, size, at in runs:
        also = corner + at
        wide = (p, cw, sw)[field]
        wide[top - away, left - size : left, :] = cl[at : at + size, :]
        wide[top - away, right : right + size, :] = cr[at : at + size, :]
        wide[low + away - 1, left - size : left, :] = cl[also : also + size, :]
        wide[low + away - 1, right : right + size, :] = cr[also : also + size, :]

    width = cols + 2 * TILE
    old, new = p, q
    for step in range(STEPS - 1):
        first, count = step + 1, rows + 2 * (STEPS - 1 - step)

        def pair(i, _, old=old, new=new, first=first):
            for k in range(2):
                r = first + 2 * i + k
                mid = old[r]
                around = pltpu.roll(mid, 1, 0) + pltpu.roll(mid, width - 1, 0)
                spread = old[r - 1] + old[r + 1] + around - 4.0 * mid
                new[r] = mid + cw[r] * spread + sw[r]
            return 0

        lax.fori_loop(0, count // 2, pair, 0)
        old, new = new, old

    def last(i, total):
        for k in range(2):
            r = top + 2 * i + k
            mid = old[r]
            around = pltpu.roll(mid, 1, 0) + pltpu.roll(mid, width - 1, 0)
            spread = old[r - 1] + old[r + 1] + around - 4.0 * mid
            later = (mid + cw[r] * spread + sw[r])[left:right]
            end[2 * i + k] = later
            total = total + later
        return total

    zero = jnp.zeros(d.shape[1:], jnp.float32)
    mean = lax.fori_loop(0, rows // 2, last, zero) * (1.0 / rows)

    def squares(i, total):
        for k in range(2):
            off = end[2 * i + k] - mean
            total = total + off * off
        return total

    stats[0] = mean
    stats[1] = lax.fori_loop(0, rows // 2, squares, zero)


def exchange(to_upper, to_lower, axis):
    count = lax.axis_size(axis)
    up = [(i, i + 1) for i in range(count - 1)]
    down = [(i + 1, i) for i in range(count - 1)]
    got = lax.ppermute(to_upper, axis, up), lax.ppermute(to_lower, axis, down)
    return [pltpu.with_memory_space_constraint(v, pltpu.VMEM) for v in got]


def combine(stats, rows):
    count = lax.axis_size("py")
    hop = 1
    while hop < count:
        group = 2 if hop == 1 or hop * 4 > count else 4
        others = [
            lax.ppermute(stats, "py", [(i, i ^ (k * hop)) for i in range(count)])
            for k in range(1, group)
        ]
        every = [stats] + others
        mean = sum(v[0] for v in every) * (1.0 / group)
        square = sum(v[1] for v in every)
        apart = sum((v[0] - mean) ** 2 for v in every)
        stats = jnp.stack([mean, square + apart * (1.0 * rows * hop)])
        hop *= group
    return stats[0], stats[1] / (rows * count)


def per_device(density, conductance, source):
    rows, cols, levels = density.shape
    f32 = jnp.float32
    _, corner = corner_runs()
    shape = pltpu.VMEM
    packs = pl.pallas_call(
        y_pack_kernel,
        out_shape=[shape((PACKED, cols, levels), f32)] * 2,
        in_specs=[pl.BlockSpec(memory_space=pl.ANY)] * 3,
        scratch_shapes=[pltpu.SemaphoreType.DMA((6,))],
        name="y_pack",
    )(density, conductance, source)
    y_got = exchange(*packs, "py")
    x_packs = pl.pallas_call(
        x_pack_kernel,
        out_shape=[shape((rows, PACKED, levels), f32)] * 2,
        name="x_pack",
    )(density, conductance, source)
    x_got = exchange(*x_packs, "px")
    corners = pl.pallas_call(
        corner_kernel,
        out_shape=[shape((2 * corner, levels), f32)] * 2,
        in_specs=[pl.BlockSpec(memory_space=pltpu.VMEM)] * 2,
        name="corners",
    )(*y_got)
    got = y_got + x_got + exchange(*corners, "px")
    wide = (rows + 2 * STEPS, cols + 2 * TILE, levels)
    end, stats = pl.pallas_call(
        step_kernel,
        out_shape=[shape(density.shape, f32), shape((2, cols, levels), f32)],
        scratch_shapes=[pltpu.VMEM(wide, f32)] * 4,
        name="steps",
    )(density, conductance, source, *got)
    mean, variance = combine(stats, rows)
    anomaly = (end - mean[None]) * lax.rsqrt(variance + 0.0001)[None]
    return (anomaly, end)


def solution(mesh):
    spec = P("py", "px", None)
    return jax.shard_map(
        per_device, mesh=mesh, in_specs=(spec,) * 3, out_specs=(spec,) * 2, check_vma=False
    )
```

```python
import jax
import jax.numpy as jnp
from jax import lax
from jax.experimental import pallas as pl
from jax.experimental.pallas import tpu as pltpu
from jax.sharding import PartitionSpec as P

STEPS = 6
LESS = STEPS - 1
TILE = 8
DEPTHS = (STEPS, LESS, LESS)
STARTS = (0, STEPS, STEPS + LESS)
PACKED = STEPS + 2 * LESS


def corner_runs():
    runs, at = [], 0
    for field, depth in enumerate(DEPTHS):
        for away in range(1, depth):
            runs.append((field, away, depth - away, at))
            at += depth - away
    return runs, -(-at // TILE) * TILE


def y_pack_kernel(d, c, s, y_hi, y_lo, sems):
    rows = d.shape[0]
    copies = []
    for ref, depth, at in zip((d, c, s), DEPTHS, STARTS):
        for out, first in ((y_hi, rows - depth), (y_lo, 0)):
            copies.append(
                pltpu.make_async_copy(
                    ref.at[pl.ds(first, depth)], out.at[pl.ds(at, depth)], sems.at[len(copies)]
                )
            )
    for copy in copies:
        copy.start()
    for copy in copies:
        copy.wait()


def x_pack_kernel(d, c, s, x_hi, x_lo, near_d, near_c, near_s):
    cols = d.shape[1]
    for ref, near, depth, at in zip((d, c, s), (near_d, near_c, near_s), DEPTHS, STARTS):
        near[...] = ref[...]
        x_hi[:, at : at + depth, :] = ref[:, cols - depth : cols, :]
        x_lo[:, at : at + depth, :] = ref[:, 0:depth, :]


def corner_kernel(from_lo, from_hi, to_right, to_left):
    cols = from_lo.shape[1]
    runs, corner = corner_runs()
    for field, away, size, at in runs:
        low = STARTS[field] + DEPTHS[field] - away
        high = STARTS[field] + away - 1
        for halo, row, to in ((from_lo, low, at), (from_hi, high, corner + at)):
            to_right[to : to + size, :] = halo[row, cols - size : cols, :]
            to_left[to : to + size, :] = halo[row, 0:size, :]


def step_kernel(
    d, c, s, from_lo, from_hi, from_left, from_right, cl, cr, end, stats, p, q, cw, sw
):
    rows, cols, _ = d.shape
    left, right = TILE, TILE + cols
    top, low = STEPS, STEPS + rows
    for ref, wide, depth, at in zip((d, c, s), (p, cw, sw), DEPTHS, STARTS):
        wide[top:low, left:right, :] = ref[...]
        wide[top - depth : top, left:right, :] = from_lo[at : at + depth]
        wide[low : low + depth, left:right, :] = from_hi[at : at + depth]
        wide[top:low, left - depth : left, :] = from_left[:, at : at + depth, :]
        wide[top:low, right : right + depth, :] = from_right[:, at : at + depth, :]
    runs, corner = corner_runs()
    for field, away, size, at in runs:
        also = corner + at
        wide = (p, cw, sw)[field]
        wide[top - away, left - size : left, :] = cl[at : at + size, :]
        wide[top - away, right : right + size, :] = cr[at : at + size, :]
        wide[low + away - 1, left - size : left, :] = cl[also : also + size, :]
        wide[low + away - 1, right : right + size, :] = cr[also : also + size, :]

    width = cols + 2 * TILE
    old, new = p, q
    for step in range(STEPS - 1):
        first, count = step + 1, rows + 2 * (STEPS - 1 - step)

        def pair(i, _, old=old, new=new, first=first):
            for k in range(2):
                r = first + 2 * i + k
                mid = old[r]
                around = pltpu.roll(mid, 1, 0) + pltpu.roll(mid, width - 1, 0)
                spread = old[r - 1] + old[r + 1] + around - 4.0 * mid
                new[r] = mid + cw[r] * spread + sw[r]
            return 0

        lax.fori_loop(0, count // 2, pair, 0)
        old, new = new, old

    def last(i, total):
        for k in range(2):
            r = top + 2 * i + k
            mid = old[r]
            around = pltpu.roll(mid, 1, 0) + pltpu.roll(mid, width - 1, 0)
            spread = old[r - 1] + old[r + 1] + around - 4.0 * mid
            later = (mid + cw[r] * spread + sw[r])[left:right]
            end[2 * i + k] = later
            total = total + later
        return total

    zero = jnp.zeros(d.shape[1:], jnp.float32)
    mean = lax.fori_loop(0, rows // 2, last, zero) * (1.0 / rows)

    def squares(i, total):
        for k in range(2):
            off = end[2 * i + k] - mean
            total = total + off * off
        return total

    stats[0] = mean
    stats[1] = lax.fori_loop(0, rows // 2, squares, zero)


def exchange(to_upper, to_lower, axis):
    count = lax.axis_size(axis)
    up = [(i, i + 1) for i in range(count - 1)]
    down = [(i + 1, i) for i in range(count - 1)]
    got = lax.ppermute(to_upper, axis, up), lax.ppermute(to_lower, axis, down)
    return [pltpu.with_memory_space_constraint(v, pltpu.VMEM) for v in got]


def combine(stats, rows):
    count = lax.axis_size("py")
    hop = 1
    while hop < count:
        group = 2 if hop == 1 or hop * 4 > count else 4
        others = [
            lax.ppermute(stats, "py", [(i, i ^ (k * hop)) for i in range(count)])
            for k in range(1, group)
        ]
        every = [stats] + others
        mean = sum(v[0] for v in every) * (1.0 / group)
        square = sum(v[1] for v in every)
        apart = sum((v[0] - mean) ** 2 for v in every)
        stats = jnp.stack([mean, square + apart * (1.0 * rows * hop)])
        hop *= group
    return stats[0], stats[1] / (rows * count)


def per_device(density, conductance, source):
    rows, cols, levels = density.shape
    f32 = jnp.float32
    _, corner = corner_runs()
    shape = pltpu.VMEM
    packs = pl.pallas_call(
        y_pack_kernel,
        out_shape=[shape((PACKED, cols, levels), f32)] * 2,
        in_specs=[pl.BlockSpec(memory_space=pl.ANY)] * 3,
        scratch_shapes=[pltpu.SemaphoreType.DMA((6,))],
        name="y_pack",
    )(density, conductance, source)
    y_got = exchange(*packs, "py")
    x_hi, x_lo, *near = pl.pallas_call(
        x_pack_kernel,
        out_shape=[shape((rows, PACKED, levels), f32)] * 2 + [shape(density.shape, f32)] * 3,
        name="x_pack",
    )(density, conductance, source)
    x_got = exchange(x_hi, x_lo, "px")
    corners = pl.pallas_call(
        corner_kernel,
        out_shape=[shape((2 * corner, levels), f32)] * 2,
        in_specs=[pl.BlockSpec(memory_space=pltpu.VMEM)] * 2,
        name="corners",
    )(*y_got)
    got = y_got + x_got + exchange(*corners, "px")
    wide = (rows + 2 * STEPS, cols + 2 * TILE, levels)
    end, stats = pl.pallas_call(
        step_kernel,
        out_shape=[shape(density.shape, f32), shape((2, cols, levels), f32)],
        in_specs=[pl.BlockSpec(memory_space=pltpu.VMEM)] * 9,
        scratch_shapes=[pltpu.VMEM(wide, f32)] * 4,
        name="steps",
    )(*[pltpu.with_memory_space_constraint(v, pltpu.VMEM) for v in near], *got)
    mean, variance = combine(stats, rows)
    anomaly = (end - mean[None]) * lax.rsqrt(variance + 0.0001)[None]
    return (anomaly, end)


def solution(mesh):
    spec = P("py", "px", None)
    return jax.shard_map(
        per_device, mesh=mesh, in_specs=(spec,) * 3, out_specs=(spec,) * 2, check_vma=False
    )
```
